32 devices in a mesh: blk: 8 (over z, x), shard: 4 (over y, core).
Axes of the slice: x: 2, y: 2, z: 4, core: 2. Of those that a mesh axis runs over, the one named last changes fastest.
Arguments:
- tokens: bfloat16 [8192, 2048], P(('blk', 'shard')), may hold values from -6 to 6
- targets: bfloat16 [8192, 2048], P(('blk', 'shard')), may hold values from -6 to 6
- up_weight: bfloat16 [2048, 7168], P(None, 'shard'), may hold values from -0.125 to 0.125
- down_weight: bfloat16 [8, 7168, 2048], P('blk', 'shard'), may hold values from -6 to 6
- mix_numer: int32 [2, 8, 3], replicated, may hold values from 1 to 2, as said below
Outputs:
- drift: bfloat16 [8, 7168, 2048], P('blk', 'shard')
The draws below stay inside these ranges and needn't reach their ends.
Inputs may be any that keep to these rules, and one draw needn't show every extreme that they name: Each row of mix_numer is (2, 1, 1), (1, 2, 1) or (1, 1, 2).
All inputs are finite; a program needn't handle non-finite values.
Results may differ from the reference program's by a relative error of at most 0.017.
Values may be sent and summed in bfloat16 or wider, within the bound.
A program may use at most 128 MiB of HBM per device.

```python
import jax
import jax.numpy as jnp
from jax import lax

D = 2048
FF = 7168
TOK = 1024
ROUNDS = 2
NW = 8


def draw_mix_numer(key, part):
    picked = jax.random.randint(key, (ROUNDS, NW), 0, 3)
    return (1 + (picked[:, :, None] == jnp.arange(3, dtype=jnp.int32)[None, None, :]).astype(jnp.int32)).astype(jnp.int32)


def levels(key, shape, shards, low, high):
    factor_of = 1.0
    for axis_at, shards_of in shards:
        steps = jax.random.uniform(jax.random.fold_in(jax.random.fold_in(key, 6), axis_at), (shards_of,), jnp.float32, low / len(shards), high / len(shards))
        factor_of = factor_of * jnp.repeat(jnp.exp(steps), shape[axis_at] // shards_of).reshape((-1,) + (1,) * (len(shape) - 1 - axis_at))
    return factor_of


def noise(rng, shape, spread, limit, cuts=(), kind=jnp.bfloat16):
    result = jax.random.normal(rng, shape, jnp.float32) * spread
    if len(cuts) > 0:
        result = levels(rng, shape, cuts, -0.22, 0.18) * result
    return jnp.clip(result, min=-limit, max=limit).astype(kind)


def setup_inputs(seed: int = 0) -> dict:
    key_list = jax.random.split(jax.random.key(seed), 6)
    tokens = noise(key_list[0], (NW * TOK, D), 1.0, 6.0, ((0, 32),))
    targets = noise(key_list[1], (NW * TOK, D), 1.0, 6.0, ((0, 32),))
    up_weight = noise(key_list[2], (D, FF), D ** -0.5, 0.125, ((1, 4),))
    down_weight = noise(key_list[3], (NW, FF, D), 1.0, 6.0, ((0, 8), (1, 4)))
    mix_numer = draw_mix_numer(jax.random.fold_in(key_list[5], 71), 0)
    return {"tokens": tokens, "targets": targets, "up_weight": up_weight, "down_weight": down_weight, "mix_numer": mix_numer}


learn_rate = 2.0

def local_step(inputs, wanted, up_weight, weight):
    hidden = jax.nn.silu(jnp.dot(inputs, up_weight, preferred_element_type=jnp.float32)).astype(jnp.bfloat16)
    output = jnp.dot(hidden, weight, preferred_element_type=jnp.float32) / jnp.sqrt(jnp.float32(FF))
    resid = (output - wanted.astype(jnp.float32)).astype(jnp.bfloat16)
    grad = jnp.dot(hidden.T, resid, preferred_element_type=jnp.float32)
    return (weight.astype(jnp.float32) - learn_rate * grad / jnp.sqrt(jnp.float32(FF))).astype(jnp.bfloat16)

def mix_round(params, numer):

    def one(index):
        left_index = (index - 1) % NW
        right_index = (index + 1) % NW
        weights = numer[index].astype(jnp.float32)
        total = weights[0] * params[index].astype(jnp.float32) + weights[1] * params[left_index].astype(jnp.float32) + weights[2] * params[right_index].astype(jnp.float32)
        return (total / 4.0).astype(jnp.bfloat16)
    return lax.map(one, jnp.arange(NW, dtype=jnp.int32))

def reference(tokens, targets, up_weight, down_weight, mix_numer):
    inputs = tokens.reshape(NW, TOK, D)
    wanted = targets.reshape(NW, TOK, D)
    stepped = lax.map(lambda item: local_step(item[0], item[1], up_weight, item[2]), (inputs, wanted, down_weight))
    mixed = stepped
    for round_index in range(ROUNDS):
        mixed = mix_round(mixed, mix_numer[round_index])

    def accumulate(index, total):
        return total + mixed[index].astype(jnp.float32)
    total = lax.fori_loop(0, NW, accumulate, jnp.zeros((FF, D), jnp.float32))
    average = total / jnp.float32(NW)
    return lax.map(lambda item: (item.astype(jnp.float32) - average).astype(jnp.bfloat16), mixed)
```

```python
import functools
import math

import jax
import jax.numpy as jnp
from jax import lax
from jax.experimental import pallas as pl
from jax.experimental.pallas import tpu as pltpu
from jax.sharding import PartitionSpec as P

learn_rate = 2.0
MESH = pl.DeviceIdType.MESH
UPTILE = 256
LAG_MIX = 3
ROWTILE = 16


def silu(v):
    return v / (1.0 + jnp.exp(-v))


def kernel(
    workers, shards, rs, cs,
    tokens, targets, up_hbm, w_hbm, numer, out,
    tok, up, w, tgt, hid, hidt, own, part, rsl, res, land,
    load_sem, tok_send, tok_recv, rs_send, rs_recv, ag_send, ag_recv,
    a2a_send, a2a_recv, ret_send, ret_recv,
):
    blk = lax.axis_index("blk")
    me = lax.axis_index("shard")
    sib = me + 1 - 2 * (me % 2)
    trows = tokens.shape[0]
    width = tokens.shape[1]
    ff = hidt.shape[0]
    chunks, chunk = w.shape[0], w.shape[2]
    pr, pc = ff // rs, chunk // cs
    far = shards // 2 - 1
    scale = jnp.float32(1.0 / math.sqrt(ff * shards))

    own_tok = pltpu.make_async_copy(tokens, tok.at[me], load_sem.at[0])
    own_tok.start()
    up_copy = pltpu.make_async_copy(up_hbm, up, load_sem.at[1])
    up_copy.start()

    barrier = pltpu.get_barrier_semaphore()

    def greet_blk(i, c):
        pl.semaphore_signal(
            barrier, inc=1, device_id={"blk": (blk + i) % workers}, device_id_type=MESH)
        return c

    lax.fori_loop(1, workers, greet_blk, 0)
    for i in range(1, shards):
        pl.semaphore_signal(
            barrier, inc=1, device_id={"shard": (me + i) % shards}, device_id_type=MESH)
    pl.semaphore_wait(barrier, workers - 1 + shards - 1)

    def tok_copy(src, which, owner, to):
        return pltpu.make_async_remote_copy(
            src_ref=src, dst_ref=tok.at[owner],
            send_sem=tok_send.at[which], recv_sem=tok_recv.at[which],
            device_id={"shard": to}, device_id_type=MESH)

    first = [tok_copy(tokens, d, me, (me + 2 * d) % shards) for d in range(1, far + 1)]
    for c in first:
        c.start()
    to_sib = tok_copy(tokens, 0, me, sib)
    to_sib.start()

    def w_copy(j):
        return pltpu.make_async_copy(
            w_hbm.at[:, pl.ds(pl.multiple_of(j * chunk, chunk), chunk)], w.at[j], load_sem.at[3 + j])

    tgt_copy = pltpu.make_async_copy(targets, tgt, load_sem.at[2])
    tgt_copy.start()
    for j in range(chunks):
        w_copy(j).start()

    def hidden_of(q):
        def tile(n, c):
            cols = pl.ds(pl.multiple_of(n * UPTILE, UPTILE), UPTILE)
            v = silu(jnp.dot(tok[q], up[:, cols], preferred_element_type=jnp.float32))
            hid[q, :, cols] = v.astype(jnp.bfloat16)
            hidt[cols, pl.ds(pl.multiple_of(q * trows, trows), trows)] = v.T.astype(jnp.bfloat16)
            return c

        lax.fori_loop(0, ff // UPTILE, tile, 0)

    own_tok.wait()
    up_copy.wait()
    hidden_of(me)
    to_sib.wait_recv()
    hidden_of(sib)
    forwards = []
    for d in range(1, far + 1):
        src = (me - 2 * d + 2 * shards) % shards
        first[d - 1].wait_recv()
        f = tok_copy(tok.at[src], far + d, src, sib)
        f.start()
        forwards.append(f)
        hidden_of(src)
    for d in range(1, far + 1):
        forwards[d - 1].wait_recv()
        hidden_of((sib - 2 * d + 2 * shards) % shards)

    tgt_copy.wait()

    def rs_copy(j, i):
        return pltpu.make_async_remote_copy(
            src_ref=part.at[j, i - 1], dst_ref=rsl.at[j, i - 1],
            send_sem=rs_send.at[j, i - 1], recv_sem=rs_recv.at[j, i - 1],
            device_id={"shard": (me + i) % shards}, device_id_type=MESH)

    def stage_out(j):
        w_copy(j).wait()

        def one(n, c):
            i = n + 1
            q = (me + i) % shards
            v = jnp.dot(hid[q], w[j], preferred_element_type=jnp.float32) * scale

            @pl.when(i < shards)
            def _():
                part[j, i - 1] = v.astype(jnp.bfloat16)
                rs_copy(j, i).start()

            @pl.when(i == shards)
            def _():
                own[j % 4] = v

            return c

        lax.fori_loop(0, shards, one, 0)

    def ag_copy(j, i):
        return pltpu.make_async_remote_copy(
            src_ref=res.at[j, me], dst_ref=res.at[j, me],
            send_sem=ag_send.at[j, i - 1], recv_sem=ag_recv.at[j, i - 1],
            device_id={"shard": (me + i) % shards}, device_id_type=MESH)

    def stage_resid(j):
        for i in range(1, shards):
            rs_copy(j, i).wait_recv()
        total = own[j % 4]
        for i in range(1, shards):
            total = total + rsl[j, i - 1].astype(jnp.float32)
        cols = pl.ds(pl.multiple_of(j * chunk, chunk), chunk)
        res[j, me] = (total - tgt[:, cols].astype(jnp.float32)).astype(jnp.bfloat16)
        for i in range(1, shards):
            ag_copy(j, i).start()

    def place(k):
        r = pl.ds(pl.multiple_of((k // cs) * pr, 16), pr)
        return r, (k % cs) * pc

    half = workers // 2
    mine = blk // half

    def peer(i):
        here = (i - 1) // half
        side = (mine + 1 + here) % 2
        return side * half + (blk + (i - 1) - here * (half - 1)) % half

    def a2a_copy(j, k, i):
        r, c0 = place(k)
        cols = pl.ds(0, pc) if cs == 1 else pl.ds(pl.multiple_of(c0, 128), pc)
        return pltpu.make_async_remote_copy(
            src_ref=w.at[j, r, cols], dst_ref=land.at[j, blk],
            send_sem=a2a_send.at[j, i], recv_sem=a2a_recv.at[j, i],
            device_id={"blk": k}, device_id_type=MESH)

    def stage_step(j):
        for i in range(1, shards):
            ag_copy(j, i).wait_recv()

        def one(n, c):
            i = n + 1
            k = peer(i)
            r, c0 = place(k)
            cols = pl.ds(0, pc) if cs == 1 else pl.ds(pl.multiple_of(c0, 128), pc)
            rhs = res[j].reshape(shards * trows, chunk) if cs == 1 else (
                res[j, :, :, cols].reshape(shards * trows, pc))
            grad = jnp.dot(hidt[r, :], rhs, preferred_element_type=jnp.float32)
            new = (w[j, r, cols].astype(jnp.float32) - (learn_rate * scale) * grad).astype(jnp.bfloat16)

            @pl.when(i < workers)
            def _():
                w[j, r, cols] = new
                a2a_copy(j, k, i).start()

            @pl.when(i == workers)
            def _():
                land[j, blk] = new

            return c

        lax.fori_loop(0, workers, one, 0)

    def out_at(j, k):
        r, c0 = place(k)
        return out.at[r, pl.ds(pl.multiple_of(j * chunk + c0, 128), pc)]

    def ret_copy(j, i):
        k = peer(i)
        return pltpu.make_async_remote_copy(
            src_ref=land.at[j, k], dst_ref=out_at(j, blk),
            send_sem=ret_send.at[j, i], recv_sem=ret_recv.at[j, i],
            device_id={"blk": k}, device_id_type=MESH)

    def own_copy(j):
        return pltpu.make_async_copy(land.at[j, blk], out_at(j, blk), ret_send.at[j, 0])

    rounds = numer.shape[1]

    def stage_mix(j):
        def arrived(i, c):
            a2a_copy(j, peer(i), i).wait_recv()
            return c

        lax.fori_loop(1, workers, arrived, 0)
        coef = [
            [[numer[e, r, k].astype(jnp.float32) * 0.25 for e in range(3)] for k in range(workers)]
            for r in range(rounds)
        ]

        def tile(t, c):
            rows = pl.ds(pl.multiple_of(t * ROWTILE, ROWTILE), ROWTILE)
            cur = [land[j, k, rows, :].astype(jnp.float32) for k in range(workers)]
            for r in range(rounds):
                cur = [
                    (
                        coef[r][k][0] * cur[k]
                        + coef[r][k][1] * cur[(k - 1) % workers]
                        + coef[r][k][2] * cur[(k + 1) % workers]
                    ).astype(jnp.bfloat16).astype(jnp.float32)
                    for k in range(workers)
                ]
            total = functools.reduce(lambda a, b: a + b, cur)
            average = total * jnp.float32(1.0 / workers)
            for k in range(workers):
                land[j, k, rows, :] = (cur[k] - average).astype(jnp.bfloat16)
            return c

        lax.fori_loop(0, pr // ROWTILE, tile, 0)

        def give(i, c):
            ret_copy(j, i).start()
            return c

        lax.fori_loop(1, workers, give, 0)
        own_copy(j).start()

    def step(t, c):
        @pl.when(t < chunks)
        def _():
            stage_out(t)

        @pl.when((t >= 1) & (t - 1 < chunks))
        def _():
            stage_step(t - 1)

        @pl.when(t < chunks)
        def _():
            stage_resid(t)

        @pl.when(t >= LAG_MIX)
        def _():
            stage_mix(t - LAG_MIX)

        return c

    lax.fori_loop(0, chunks + LAG_MIX, step, 0)

    to_sib.wait_send()
    for c in first + forwards:
        c.wait_send()

    def finish(j, c):
        for i in range(1, shards):
            rs_copy(j, i).wait_send()
            ag_copy(j, i).wait_send()

        def one(i, c):
            a2a_copy(j, peer(i), i).wait_send()
            r = ret_copy(j, i)
            r.wait_send()
            r.wait_recv()
            return c

        lax.fori_loop(1, workers, one, 0)
        own_copy(j).wait()
        return c

    lax.fori_loop(0, chunks, finish, 0)


def solution(mesh):
    workers, shards = mesh.shape["blk"], mesh.shape["shard"]

    def body(tokens, targets, up_weight, down_weight, mix_numer):
        weight = down_weight[0]
        ff, d = weight.shape
        trows = tokens.shape[0]

        rs = math.gcd(workers, ff // 16)
        cs = workers // rs
        chunk = 128 * cs
        chunks = d // chunk
        pr, pc = ff // rs, chunk // cs
        far = shards // 2 - 1
        bf = jnp.bfloat16
        dma = pltpu.SemaphoreType.DMA
        any_ref = pl.BlockSpec(memory_space=pltpu.HBM)
        out = pl.pallas_call(
            functools.partial(kernel, workers, shards, rs, cs),
            out_shape=pltpu.VMEM((ff, d), bf),
            in_specs=[any_ref] * 4 + [pl.BlockSpec(memory_space=pltpu.SMEM)],
            out_specs=pl.BlockSpec(memory_space=pltpu.VMEM),
            scratch_shapes=[
                pltpu.VMEM((shards, trows, d), bf),
                pltpu.VMEM((d, ff), bf),
                pltpu.VMEM((chunks, ff, chunk), bf),
                pltpu.VMEM((trows, d), bf),
                pltpu.VMEM((shards, trows, ff), bf),
                pltpu.VMEM((ff, shards * trows), bf),
                pltpu.VMEM((4, trows, chunk), jnp.float32),
                pltpu.VMEM((chunks, shards - 1, trows, chunk), bf),
                pltpu.VMEM((chunks, shards - 1, trows, chunk), bf),
                pltpu.VMEM((chunks, shards, trows, chunk), bf),
                pltpu.VMEM((chunks, workers, pr, pc), bf),
                dma((3 + chunks,)),
                dma((2 * far + 1,)),
                dma((2 * far + 1,)),
                dma((chunks, shards - 1)),
                dma((chunks, shards - 1)),
                dma((chunks, shards - 1)),
                dma((chunks, shards - 1)),
                dma((chunks, workers)),
                dma((chunks, workers)),
                dma((chunks, workers)),
                dma((chunks, workers)),
            ],
            compiler_params=pltpu.CompilerParams(
                collective_id=0, has_side_effects=True, vmem_limit_bytes=54 * 1024 * 1000
            ),
        )(tokens, targets, up_weight, weight, jnp.transpose(mix_numer, (2, 0, 1)))
        return out[None]

    in_specs = (
        P(("blk", "shard"), None),
        P(("blk", "shard"), None),
        P(None, "shard"),
        P("blk", "shard", None),
        P(),
    )
    return jax.shard_map(
        body, mesh=mesh, in_specs=in_specs, out_specs=P("blk", "shard", None), check_vma=False
    )
```

```python
import functools
import math

import jax
import jax.numpy as jnp
from jax import lax
from jax.experimental import pallas as pl
from jax.experimental.pallas import tpu as pltpu
from jax.sharding import PartitionSpec as P

learn_rate = 2.0
MESH = pl.DeviceIdType.MESH
UPTILE = 256
LAG_MIX = 3
ROWTILE = 16


def silu(v):
    return v / (1.0 + jnp.exp(-v))


def kernel(
    workers, shards, rs, cs,
    tokens, targets, up_hbm, w_hbm, numer, out,
    tok, up, w, tgt, hid, hidt, own, part, rsl, res, land,
    load_sem, tok_send, tok_recv, rs_send, rs_recv, ag_send, ag_recv,
    a2a_send, a2a_recv, ret_send, ret_recv, own_sem,
):
    blk = lax.axis_index("blk")
    me = lax.axis_index("shard")
    sib = me + 1 - 2 * (me % 2)
    trows = tokens.shape[0]
    width = tokens.shape[1]
    ff = hidt.shape[0]
    chunks, chunk = w.shape[0], w.shape[2]
    pr, pc = ff // rs, chunk // cs
    far = shards // 2 - 1
    scale = jnp.float32(1.0 / math.sqrt(ff * shards))

    own_tok = pltpu.make_async_copy(tokens, tok.at[me], load_sem.at[0])
    own_tok.start()
    up_copy = pltpu.make_async_copy(up_hbm, up, load_sem.at[1])
    up_copy.start()

    barrier = pltpu.get_barrier_semaphore()

    def await_bytes(ref, sem):
        pltpu.make_async_copy(ref, ref, sem).wait()

    def greet_blk(i, c):
        pl.semaphore_signal(
            barrier, inc=1, device_id={"blk": (blk + i) % workers}, device_id_type=MESH)
        return c

    lax.fori_loop(1, workers, greet_blk, 0)
    for i in range(1, shards):
        pl.semaphore_signal(
            barrier, inc=1, device_id={"shard": (me + i) % shards}, device_id_type=MESH)
    pl.semaphore_wait(barrier, workers - 1 + shards - 1)

    def tok_copy(src, which, owner, to):
        return pltpu.make_async_remote_copy(
            src_ref=src, dst_ref=tok.at[owner],
            send_sem=tok_send.at[which], recv_sem=tok_recv.at[which],
            device_id={"shard": to}, device_id_type=MESH)

    first = [tok_copy(tokens, d, me, (me + 2 * d) % shards) for d in range(1, far + 1)]
    for c in first:
        c.start()
    to_sib = tok_copy(tokens, 0, me, sib)
    to_sib.start()

    def w_copy(j):
        return pltpu.make_async_copy(
            w_hbm.at[:, pl.ds(pl.multiple_of(j * chunk, chunk), chunk)], w.at[j], load_sem.at[3 + j])

    tgt_copy = pltpu.make_async_copy(targets, tgt, load_sem.at[2])
    tgt_copy.start()
    for j in range(chunks):
        w_copy(j).start()

    def hidden_of(q):
        def tile(n, c):
            cols = pl.ds(pl.multiple_of(n * UPTILE, UPTILE), UPTILE)
            v = silu(jnp.dot(tok[q], up[:, cols], preferred_element_type=jnp.float32))
            hid[q, :, cols] = v.astype(jnp.bfloat16)
            hidt[cols, pl.ds(pl.multiple_of(q * trows, trows), trows)] = v.T.astype(jnp.bfloat16)
            return c

        lax.fori_loop(0, ff // UPTILE, tile, 0)

    own_tok.wait()
    up_copy.wait()
    hidden_of(me)
    to_sib.wait_recv()
    hidden_of(sib)
    forwards = []
    for d in range(1, far + 1):
        src = (me - 2 * d + 2 * shards) % shards
        first[d - 1].wait_recv()
        f = tok_copy(tok.at[src], far + d, src, sib)
        f.start()
        forwards.append(f)
        hidden_of(src)
    for d in range(1, far + 1):
        forwards[d - 1].wait_recv()
        hidden_of((sib - 2 * d + 2 * shards) % shards)

    tgt_copy.wait()

    def rs_copy(j, i):
        return pltpu.make_async_remote_copy(
            src_ref=part.at[j, i - 1], dst_ref=rsl.at[j, i - 1],
            send_sem=rs_send.at[0], recv_sem=rs_recv.at[j],
            device_id={"shard": (me + i) % shards}, device_id_type=MESH)

    def stage_out(j):
        w_copy(j).wait()

        def one(n, c):
            i = n + 1
            q = (me + i) % shards
            v = jnp.dot(hid[q], w[j], preferred_element_type=jnp.float32) * scale

            @pl.when(i < shards)
            def _():
                part[j, i - 1] = v.astype(jnp.bfloat16)
                rs_copy(j, i).start()

            @pl.when(i == shards)
            def _():
                own[j % 4] = v

            return c

        lax.fori_loop(0, shards, one, 0)

    def ag_copy(j, i):
        return pltpu.make_async_remote_copy(
            src_ref=res.at[j, me], dst_ref=res.at[j, me],
            send_sem=ag_send.at[0], recv_sem=ag_recv.at[j],
            device_id={"shard": (me + i) % shards}, device_id_type=MESH)

    def stage_resid(j):
        await_bytes(rsl.at[j], rs_recv.at[j])
        total = own[j % 4]
        for i in range(1, shards):
            total = total + rsl[j, i - 1].astype(jnp.float32)
        cols = pl.ds(pl.multiple_of(j * chunk, chunk), chunk)
        res[j, me] = (total - tgt[:, cols].astype(jnp.float32)).astype(jnp.bfloat16)
        for i in range(1, shards):
            ag_copy(j, i).start()

    def place(k):
        r = pl.ds(pl.multiple_of((k // cs) * pr, 16), pr)
        return r, (k % cs) * pc

    half = workers // 2
    mine = blk // half

    def peer(i):
        here = (i - 1) // half
        side = (mine + 1 + here) % 2
        return side * half + (blk + (i - 1) - here * (half - 1)) % half

    def a2a_copy(j, k, i):
        r, c0 = place(k)
        cols = pl.ds(0, pc) if cs == 1 else pl.ds(pl.multiple_of(c0, 128), pc)
        return pltpu.make_async_remote_copy(
            src_ref=w.at[j, r, cols], dst_ref=land.at[j, blk],
            send_sem=a2a_send.at[0], recv_sem=a2a_recv.at[j],
            device_id={"blk": k}, device_id_type=MESH)

    def stage_step(j):
        await_bytes(res.at[j, pl.ds(0, shards - 1)], ag_recv.at[j])

        def one(n, c):
            i = n + 1
            k = peer(i)
            r, c0 = place(k)
            cols = pl.ds(0, pc) if cs == 1 else pl.ds(pl.multiple_of(c0, 128), pc)
            rhs = res[j].reshape(shards * trows, chunk) if cs == 1 else (
                res[j, :, :, cols].reshape(shards * trows, pc))
            grad = jnp.dot(hidt[r, :], rhs, preferred_element_type=jnp.float32)
            new = (w[j, r, cols].astype(jnp.float32) - (learn_rate * scale) * grad).astype(jnp.bfloat16)

            @pl.when(i < workers)
            def _():
                w[j, r, cols] = new
                a2a_copy(j, k, i).start()

            @pl.when(i == workers)
            def _():
                land[j, blk] = new

            return c

        lax.fori_loop(0, workers, one, 0)

    def out_at(j, k):
        r, c0 = place(k)
        return out.at[r, pl.ds(pl.multiple_of(j * chunk + c0, 128), pc)]

    def ret_copy(j, i):
        k = peer(i)
        return pltpu.make_async_remote_copy(
            src_ref=land.at[j, k], dst_ref=out_at(j, blk),
            send_sem=ret_send.at[0], recv_sem=ret_recv.at[0],
            device_id={"blk": k}, device_id_type=MESH)

    def own_copy(j):
        return pltpu.make_async_copy(land.at[j, blk], out_at(j, blk), own_sem.at[0])

    rounds = numer.shape[1]

    def stage_mix(j):
        await_bytes(land.at[j, pl.ds(0, workers - 1)], a2a_recv.at[j])
        coef = [
            [[numer[e, r, k].astype(jnp.float32) * 0.25 for e in range(3)] for k in range(workers)]
            for r in range(rounds)
        ]

        def tile(t, c):
            rows = pl.ds(pl.multiple_of(t * ROWTILE, ROWTILE), ROWTILE)
            cur = [land[j, k, rows, :].astype(jnp.float32) for k in range(workers)]
            for r in range(rounds):
                cur = [
                    (
                        coef[r][k][0] * cur[k]
                        + coef[r][k][1] * cur[(k - 1) % workers]
                        + coef[r][k][2] * cur[(k + 1) % workers]
                    ).astype(jnp.bfloat16).astype(jnp.float32)
                    for k in range(workers)
                ]
            total = functools.reduce(lambda a, b: a + b, cur)
            average = total * jnp.float32(1.0 / workers)
            for k in range(workers):
                land[j, k, rows, :] = (cur[k] - average).astype(jnp.bfloat16)
            return c

        lax.fori_loop(0, pr // ROWTILE, tile, 0)

        def give(i, c):
            ret_copy(j, i).start()
            return c

        lax.fori_loop(1, workers, give, 0)
        own_copy(j).start()

    def step(t, c):
        @pl.when(t < chunks)
        def _():
            stage_out(t)

        @pl.when((t >= 1) & (t - 1 < chunks))
        def _():
            stage_step(t - 1)

        @pl.when(t < chunks)
        def _():
            stage_resid(t)

        @pl.when(t >= LAG_MIX)
        def _():
            stage_mix(t - LAG_MIX)

        return c

    lax.fori_loop(0, chunks + LAG_MIX, step, 0)

    to_sib.wait_send()
    for c in first + forwards:
        c.wait_send()

    await_bytes(part, rs_send.at[0])
    await_bytes(res.at[:, pl.ds(0, shards - 1)], ag_send.at[0])
    away = land.at[:, pl.ds(0, workers - 1)]
    await_bytes(away, a2a_send.at[0])
    await_bytes(away, ret_send.at[0])
    await_bytes(away, ret_recv.at[0])
    await_bytes(land.at[:, 0], own_sem.at[0])


def solution(mesh):
    workers, shards = mesh.shape["blk"], mesh.shape["shard"]

    def body(tokens, targets, up_weight, down_weight, mix_numer):
        weight = down_weight[0]
        ff, d = weight.shape
        trows = tokens.shape[0]

        rs = math.gcd(workers, ff // 16)
        cs = workers // rs
        chunk = 128 * cs
        chunks = d // chunk
        pr, pc = ff // rs, chunk // cs
        far = shards // 2 - 1
        bf = jnp.bfloat16
        dma = pltpu.SemaphoreType.DMA
        any_ref = pl.BlockSpec(memory_space=pltpu.HBM)
        out = pl.pallas_call(
            functools.partial(kernel, workers, shards, rs, cs),
            out_shape=pltpu.VMEM((ff, d), bf),
            in_specs=[any_ref] * 4 + [pl.BlockSpec(memory_space=pltpu.SMEM)],
            out_specs=pl.BlockSpec(memory_space=pltpu.VMEM),
            scratch_shapes=[
                pltpu.VMEM((shards, trows, d), bf),
                pltpu.VMEM((d, ff), bf),
                pltpu.VMEM((chunks, ff, chunk), bf),
                pltpu.VMEM((trows, d), bf),
                pltpu.VMEM((shards, trows, ff), bf),
                pltpu.VMEM((ff, shards * trows), bf),
                pltpu.VMEM((4, trows, chunk), jnp.float32),
                pltpu.VMEM((chunks, shards - 1, trows, chunk), bf),
                pltpu.VMEM((chunks, shards - 1, trows, chunk), bf),
                pltpu.VMEM((chunks, shards, trows, chunk), bf),
                pltpu.VMEM((chunks, workers, pr, pc), bf),
                dma((3 + chunks,)),
                dma((2 * far + 1,)),
                dma((2 * far + 1,)),
                dma((1,)),
                dma((chunks,)),
                dma((1,)),
                dma((chunks,)),
                dma((1,)),
                dma((chunks,)),
                dma((1,)),
                dma((1,)),
                dma((1,)),
            ],
            compiler_params=pltpu.CompilerParams(
                collective_id=0, has_side_effects=True, vmem_limit_bytes=54 * 1024 * 1000
            ),
        )(tokens, targets, up_weight, weight, jnp.transpose(mix_numer, (2, 0, 1)))
        return out[None]

    in_specs = (
        P(("blk", "shard"), None),
        P(("blk", "shard"), None),
        P(None, "shard"),
        P("blk", "shard", None),
        P(),
    )
    return jax.shard_map(
        body, mesh=mesh, in_specs=in_specs, out_specs=P("blk", "shard", None), check_vma=False
    )
```

```python
import functools
import math

import jax
import jax.numpy as jnp
from jax import lax
from jax.experimental import pallas as pl
from jax.experimental.pallas import tpu as pltpu
from jax.sharding import PartitionSpec as P

learn_rate = 2.0
MESH = pl.DeviceIdType.MESH
UPTILE = 256
LAG_MIX = 4
PIECES = 8
HELPED = 3
EARLY = 3
ROWTILE = 16


def silu(v):
    return v / (1.0 + jnp.exp(-v))


def kernel(
    workers, shards, rs, cs,
    tokens, targets, up_hbm, w_hbm, numer, out,
    tok, up, w, tgt, hid, hidt, own, part, rsl, res, land, relay,
    load_sem, tok_send, tok_recv, help_send, help_recv, rs_send, rs_recv, ag_send, ag_recv,
    a2a_send, a2a_recv, ret_send, ret_recv, own_sem,
):
    blk = lax.axis_index("blk")
    me = lax.axis_index("shard")
    sib = me + 1 - 2 * (me % 2)
    trows = tokens.shape[0]
    width = tokens.shape[1]
    ff = hidt.shape[0]
    chunks, chunk = w.shape[0], w.shape[2]
    pr, pc = ff // rs, chunk // cs
    far = shards // 2 - 1
    scale = jnp.float32(1.0 / math.sqrt(ff * shards))

    own_tok = pltpu.make_async_copy(tokens, tok.at[me], load_sem.at[0])
    own_tok.start()
    up_copy = pltpu.make_async_copy(up_hbm, up, load_sem.at[1])
    up_copy.start()

    barrier = pltpu.get_barrier_semaphore()

    def await_bytes(ref, sem):
        pltpu.make_async_copy(ref, ref, sem).wait()

    def greet_blk(i, c):
        pl.semaphore_signal(
            barrier, inc=1, device_id={"blk": (blk + i) % workers}, device_id_type=MESH)
        return c

    lax.fori_loop(1, workers, greet_blk, 0)
    for i in range(1, shards):
        pl.semaphore_signal(
            barrier, inc=1, device_id={"shard": (me + i) % shards}, device_id_type=MESH)
    quarter = workers // 4
    helped = HELPED if workers % 4 == 0 and far == 1 else 0
    inner = (blk >= quarter) & (blk < workers - quarter)
    aside = jnp.where(blk < workers // 2, quarter, -quarter)
    helper = {"blk": blk + jnp.where(inner, -aside, aside), "shard": (me + 2) % shards}
    if helped:
        pl.semaphore_signal(barrier, inc=1, device_id=helper, device_id_type=MESH)
    pl.semaphore_wait(barrier, workers - 1 + shards - 1 + (1 if helped else 0))

    prow = trows // PIECES

    def rows_of(p):
        return pl.ds(p * prow, prow)

    def tok_copy(src, sem, owner, p, to):
        return pltpu.make_async_remote_copy(
            src_ref=src.at[rows_of(p)], dst_ref=tok.at[owner, rows_of(p)],
            send_sem=tok_send.at[0], recv_sem=tok_recv.at[sem],
            device_id={"shard": to}, device_id_type=MESH)

    def direct(d, p):
        return tok_copy(tokens, 1 + (2 * d - 2) * PIECES + p, me, p, (me + 2 * d) % shards)

    def forward(d, p):
        src = (me - 2 * d + 2 * shards) % shards
        return tok_copy(tok.at[src], 1 + (2 * d - 1) * PIECES + p, src, p, sib)

    def to_relay(p):
        return pltpu.make_async_remote_copy(
            src_ref=tokens.at[rows_of(p)], dst_ref=relay.at[p - PIECES + helped],
            send_sem=tok_send.at[0], recv_sem=help_recv.at[p - PIECES + helped],
            device_id=helper, device_id_type=MESH)

    def from_relay(p):
        owner = (me + 2) % shards
        return pltpu.make_async_remote_copy(
            src_ref=relay.at[p - PIECES + helped], dst_ref=tok.at[owner, rows_of(p)],
            send_sem=help_send.at[0], recv_sem=tok_recv.at[1 + p],
            device_id={"blk": blk + aside}, device_id_type=MESH)

    sib_copy = pltpu.make_async_remote_copy(
        src_ref=tokens, dst_ref=tok.at[me], send_sem=tok_send.at[0], recv_sem=tok_recv.at[0],
        device_id={"shard": sib}, device_id_type=MESH)

    def send_direct(last):
        for p in range(last):
            for d in range(1, far + 1):
                direct(d, p).start()

    if helped:
        @pl.when(inner)
        def _():
            for p in range(PIECES - helped, PIECES):
                to_relay(p).start()
            send_direct(PIECES - helped)
    else:
        send_direct(PIECES)
    sib_copy.start()

    def w_copy(j):
        return pltpu.make_async_copy(
            w_hbm.at[:, pl.ds(pl.multiple_of(j * chunk, chunk), chunk)], w.at[j], load_sem.at[3 + j])

    tgt_copy = pltpu.make_async_copy(targets, tgt, load_sem.at[2])
    tgt_copy.start()
    for j in range(chunks):
        w_copy(j).start()

    def hidden_of(q, r0, n):
        def tile(t, c):
            cols = pl.ds(pl.multiple_of(t * UPTILE, UPTILE), UPTILE)
            v = silu(jnp.dot(tok[q, r0:r0 + n], up[:, cols], preferred_element_type=jnp.float32))
            hid[q, r0:r0 + n, cols] = v.astype(jnp.bfloat16)
            hidt[cols, pl.ds(pl.multiple_of(q * trows + r0, 128), n)] = v.T.astype(jnp.bfloat16)
            return c

        lax.fori_loop(0, ff // UPTILE, tile, 0, unroll=True)

    def rs_copy(j, i):
        return pltpu.make_async_remote_copy(
            src_ref=part.at[j, i - 1], dst_ref=rsl.at[j, i - 1],
            send_sem=rs_send.at[0], recv_sem=rs_recv.at[j],
            device_id={"shard": (me + i) % shards}, device_id_type=MESH)

    near = (sib - me + shards) % shards

    def out_of(q, j):
        return jnp.dot(hid[q], w[j], preferred_element_type=jnp.float32) * scale

    def give_out(j, i):
        part[j, i - 1] = out_of((me + i) % shards, j).astype(jnp.bfloat16)
        rs_copy(j, i).start()

    def out_away(j):
        def one(n, c):
            give_out(j, 1 + n + jnp.where(n + 1 >= near, 1, 0))
            return c

        lax.fori_loop(0, shards - 2, one, 0)

    def out_here(j):
        give_out(j, near)
        own[j % 4] = out_of(me, j)

    def relay_one(p):
        if helped:
            @pl.when(jnp.logical_not(inner))
            def _():
                to_relay(p).wait_recv()
                from_relay(p).start()

    def pass_on(pieces):
        for p in pieces:
            for d in range(1, far + 1):
                direct(d, p).wait_recv()
                forward(d, p).start()

    def passed_on(pieces):
        for p in pieces:
            for d in range(1, far + 1):
                forward(d, p).wait_recv()

    own_tok.wait()
    up_copy.wait()
    hidden_of(me, 0, trows)
    for p in range(PIECES - helped, PIECES - 1):
        relay_one(p)
    sib_copy.wait_recv()
    hidden_of(sib, 0, trows)
    if helped:
        relay_one(PIECES - 1)

        @pl.when(jnp.logical_not(inner))
        def _():
            send_direct(PIECES)

    h = PIECES // 2
    for j in range(EARLY):
        w_copy(j).wait()
        out_here(j)
        pass_on(range(h * j // EARLY, h * (j + 1) // EARLY))
    mid = trows // 2
    for d in range(1, far + 1):
        hidden_of((me - 2 * d + 2 * shards) % shards, 0, mid)
    passed_on(range(h))
    for d in range(1, far + 1):
        hidden_of((sib - 2 * d + 2 * shards) % shards, 0, mid)
    pass_on(range(h, PIECES))
    for d in range(1, far + 1):
        hidden_of((me - 2 * d + 2 * shards) % shards, mid, trows - mid)
    passed_on(range(h, PIECES))
    for d in range(1, far + 1):
        hidden_of((sib - 2 * d + 2 * shards) % shards, mid, trows - mid)

    tgt_copy.wait()

    def ag_copy(j, i):
        return pltpu.make_async_remote_copy(
            src_ref=res.at[j, me], dst_ref=res.at[j, me],
            send_sem=ag_send.at[0], recv_sem=ag_recv.at[j],
            device_id={"shard": (me + i) % shards}, device_id_type=MESH)

    def stage_resid(j):
        await_bytes(rsl.at[j], rs_recv.at[j])
        total = own[j % 4]
        for i in range(1, shards):
            total = total + rsl[j, i - 1].astype(jnp.float32)
        cols = pl.ds(pl.multiple_of(j * chunk, chunk), chunk)
        res[j, me] = (total - tgt[:, cols].astype(jnp.float32)).astype(jnp.bfloat16)
        for i in range(1, shards):
            ag_copy(j, i).start()

    def place(k):
        r = pl.ds(pl.multiple_of((k // cs) * pr, 16), pr)
        return r, (k % cs) * pc

    half = workers // 2
    mine = blk // half

    def peer(i):
        here = (i - 1) // half
        side = (mine + 1 + here) % 2
        return side * half + (blk + (i - 1) - here * (half - 1)) % half

    def a2a_copy(j, k, i):
        r, c0 = place(k)
        cols = pl.ds(0, pc) if cs == 1 else pl.ds(pl.multiple_of(c0, 128), pc)
        return pltpu.make_async_remote_copy(
            src_ref=w.at[j, r, cols], dst_ref=land.at[j, blk],
            send_sem=a2a_send.at[0], recv_sem=a2a_recv.at[j],
            device_id={"blk": k}, device_id_type=MESH)

    def stage_step(j):
        await_bytes(res.at[j, pl.ds(0, shards - 1)], ag_recv.at[j])

        def one(n, c):
            i = n + 1
            k = peer(i)
            r, c0 = place(k)
            cols = pl.ds(0, pc) if cs == 1 else pl.ds(pl.multiple_of(c0, 128), pc)
            rhs = res[j].reshape(shards * trows, chunk) if cs == 1 else (
                res[j, :, :, cols].reshape(shards * trows, pc))
            grad = jnp.dot(hidt[r, :], rhs, preferred_element_type=jnp.float32)
            new = (w[j, r, cols].astype(jnp.float32) - (learn_rate * scale) * grad).astype(jnp.bfloat16)

            @pl.when(i < workers)
            def _():
                w[j, r, cols] = new
                a2a_copy(j, k, i).start()

            @pl.when(i == workers)
            def _():
                land[j, blk] = new

            return c

        lax.fori_loop(0, workers, one, 0)

    def out_at(j, k):
        r, c0 = place(k)
        return out.at[r, pl.ds(pl.multiple_of(j * chunk + c0, 128), pc)]

    def ret_copy(j, i):
        k = peer(i)
        return pltpu.make_async_remote_copy(
            src_ref=land.at[j, k], dst_ref=out_at(j, blk),
            send_sem=ret_send.at[0], recv_sem=ret_recv.at[0],
            device_id={"blk": k}, device_id_type=MESH)

    def own_copy(j):
        return pltpu.make_async_copy(land.at[j, blk], out_at(j, blk), own_sem.at[0])

    rounds = numer.shape[1]

    def stage_mix(j):
        await_bytes(land.at[j, pl.ds(0, workers - 1)], a2a_recv.at[j])
        coef = [
            [[numer[e, r, k].astype(jnp.float32) * 0.25 for e in range(3)] for k in range(workers)]
            for r in range(rounds)
        ]

        def tile(t, c):
            rows = pl.ds(pl.multiple_of(t * ROWTILE, ROWTILE), ROWTILE)
            cur = [land[j, k, rows, :].astype(jnp.float32) for k in range(workers)]
            for r in range(rounds):
                cur = [
                    (
                        coef[r][k][0] * cur[k]
                        + coef[r][k][1] * cur[(k - 1) % workers]
                        + coef[r][k][2] * cur[(k + 1) % workers]
                    ).astype(jnp.bfloat16).astype(jnp.float32)
                    for k in range(workers)
                ]
            total = functools.reduce(lambda a, b: a + b, cur)
            average = total * jnp.float32(1.0 / workers)
            for k in range(workers):
                land[j, k, rows, :] = (cur[k] - average).astype(jnp.bfloat16)
            return c

        lax.fori_loop(0, pr // ROWTILE, tile, 0)

        def give(i, c):
            ret_copy(j, i).start()
            return c

        lax.fori_loop(1, workers, give, 0)
        own_copy(j).start()

    def step(t, c):
        @pl.when((t < chunks) & (t >= EARLY))
        def _():
            w_copy(t).wait()

        @pl.when(t < chunks)
        def _():
            out_away(t)

        @pl.when((t < chunks) & (t >= EARLY))
        def _():
            out_here(t)

        @pl.when((t >= 1) & (t - 1 < chunks))
        def _():
            stage_step(t - 1)

        @pl.when(t < chunks)
        def _():
            stage_resid(t)

        @pl.when(t >= LAG_MIX)
        def _():
            stage_mix(t - LAG_MIX)

        return c

    lax.fori_loop(0, chunks + LAG_MIX, step, 0)

    await_bytes(tok.at[pl.ds(0, 2 * far + 1)], tok_send.at[0])
    if helped:
        @pl.when(jnp.logical_not(inner))
        def _():
            await_bytes(relay, help_send.at[0])

    await_bytes(part, rs_send.at[0])
    await_bytes(res.at[:, pl.ds(0, shards - 1)], ag_send.at[0])
    away = land.at[:, pl.ds(0, workers - 1)]
    await_bytes(away, a2a_send.at[0])
    await_bytes(away, ret_send.at[0])
    await_bytes(away, ret_recv.at[0])
    await_bytes(land.at[:, 0], own_sem.at[0])


def solution(mesh):
    workers, shards = mesh.shape["blk"], mesh.shape["shard"]

    def body(tokens, targets, up_weight, down_weight, mix_numer):
        weight = down_weight[0]
        ff, d = weight.shape
        trows = tokens.shape[0]

        rs = math.gcd(workers, ff // 16)
        cs = workers // rs
        chunk = 128 * cs
        chunks = d // chunk
        pr, pc = ff // rs, chunk // cs
        far = shards // 2 - 1
        bf = jnp.bfloat16
        dma = pltpu.SemaphoreType.DMA
        any_ref = pl.BlockSpec(memory_space=pltpu.HBM)
        out = pl.pallas_call(
            functools.partial(kernel, workers, shards, rs, cs),
            out_shape=pltpu.VMEM((ff, d), bf),
            in_specs=[any_ref] * 4 + [pl.BlockSpec(memory_space=pltpu.SMEM)],
            out_specs=pl.BlockSpec(memory_space=pltpu.VMEM),
            scratch_shapes=[
                pltpu.VMEM((shards, trows, d), bf),
                pltpu.VMEM((d, ff), bf),
                pltpu.VMEM((chunks, ff, chunk), bf),
                pltpu.VMEM((trows, d), bf),
                pltpu.VMEM((shards, trows, ff), bf),
                pltpu.VMEM((ff, shards * trows), bf),
                pltpu.VMEM((4, trows, chunk), jnp.float32),
                pltpu.VMEM((chunks, shards - 1, trows, chunk), bf),
                pltpu.VMEM((chunks, shards - 1, trows, chunk), bf),
                pltpu.VMEM((chunks, shards, trows, chunk), bf),
                pltpu.VMEM((chunks, workers, pr, pc), bf),
                pltpu.VMEM((HELPED, trows // PIECES, d), bf),
                dma((3 + chunks,)),
                dma((1,)),
                dma((1 + 2 * far * PIECES,)),
                dma((1,)),
                dma((HELPED,)),
                dma((1,)),
                dma((chunks,)),
                dma((1,)),
                dma((chunks,)),
                dma((1,)),
                dma((chunks,)),
                dma((1,)),
                dma((1,)),
                dma((1,)),
            ],
            compiler_params=pltpu.CompilerParams(
                collective_id=0, has_side_effects=True, vmem_limit_bytes=54 * 1024 * 1000
            ),
        )(tokens, targets, up_weight, weight, jnp.transpose(mix_numer, (2, 0, 1)))
        return out[None]

    in_specs = (
        P(("blk", "shard"), None),
        P(("blk", "shard"), None),
        P(None, "shard"),
        P("blk", "shard", None),
        P(),
    )
    return jax.shard_map(
        body, mesh=mesh, in_specs=in_specs, out_specs=P("blk", "shard", None), check_vma=False
    )
```

```python
import functools
import math

import jax
import jax.numpy as jnp
from jax import lax
from jax.experimental import pallas as pl
from jax.experimental.pallas import tpu as pltpu
from jax.sharding import PartitionSpec as P

learn_rate = 2.0
MESH = pl.DeviceIdType.MESH
UPTILE = 256
LAG_MIX = 4
PIECES = 8
HELPED = 3
EARLY = 2
ROWTILE = 16


def silu(v):
    return v / (1.0 + jnp.exp(-v))


def kernel(
    workers, shards, rs, cs,
    tokens, targets, up_hbm, w_hbm, numer, out,
    tok, up, w, tgt, hid, hidt, own, part, rsl, res, land, relay,
    load_sem, tok_send, tok_recv, help_send, help_recv, rs_send, rs_recv, ag_send, ag_recv,
    a2a_send, a2a_recv, ret_send, ret_recv, own_sem,
):
    blk = lax.axis_index("blk")
    me = lax.axis_index("shard")
    sib = me + 1 - 2 * (me % 2)
    trows = tokens.shape[0]
    width = tokens.shape[1]
    ff = hidt.shape[0]
    chunks, chunk = w.shape[0], w.shape[2]
    pr, pc = ff // rs, chunk // cs
    far = shards // 2 - 1
    scale = jnp.float32(1.0 / math.sqrt(ff * shards))

    own_tok = pltpu.make_async_copy(tokens, tok.at[me], load_sem.at[0])
    own_tok.start()
    up_copy = pltpu.make_async_copy(up_hbm, up, load_sem.at[1])
    up_copy.start()

    barrier = pltpu.get_barrier_semaphore()

    def await_bytes(ref, sem):
        pltpu.make_async_copy(ref, ref, sem).wait()

    def greet_blk(i, c):
        pl.semaphore_signal(
            barrier, inc=1, device_id={"blk": (blk + i) % workers}, device_id_type=MESH)
        return c

    lax.fori_loop(1, workers, greet_blk, 0)
    for i in range(1, shards):
        pl.semaphore_signal(
            barrier, inc=1, device_id={"shard": (me + i) % shards}, device_id_type=MESH)
    quarter = workers // 4
    helped = HELPED if workers % 4 == 0 and far == 1 else 0
    inner = (blk >= quarter) & (blk < workers - quarter)
    aside = jnp.where(blk < workers // 2, quarter, -quarter)
    helper = {"blk": blk + jnp.where(inner, -aside, aside), "shard": (me + 2) % shards}
    if helped:
        pl.semaphore_signal(barrier, inc=1, device_id=helper, device_id_type=MESH)
    pl.semaphore_wait(barrier, workers - 1 + shards - 1 + (1 if helped else 0))

    prow = trows // PIECES

    def rows_of(p):
        return pl.ds(p * prow, prow)

    def tok_copy(src, sem, owner, p, to):
        return pltpu.make_async_remote_copy(
            src_ref=src.at[rows_of(p)], dst_ref=tok.at[owner, rows_of(p)],
            send_sem=tok_send.at[0], recv_sem=tok_recv.at[sem],
            device_id={"shard": to}, device_id_type=MESH)

    def direct(d, p):
        return tok_copy(tokens, 1 + (2 * d - 2) * PIECES + p, me, p, (me + 2 * d) % shards)

    def forward(d, p):
        src = (me - 2 * d + 2 * shards) % shards
        return tok_copy(tok.at[src], 1 + (2 * d - 1) * PIECES + p, src, p, sib)

    def to_relay(p):
        return pltpu.make_async_remote_copy(
            src_ref=tokens.at[rows_of(p)], dst_ref=relay.at[p - PIECES + helped],
            send_sem=tok_send.at[0], recv_sem=help_recv.at[p - PIECES + helped],
            device_id=helper, device_id_type=MESH)

    def from_relay(p):
        owner = (me + 2) % shards
        return pltpu.make_async_remote_copy(
            src_ref=relay.at[p - PIECES + helped], dst_ref=tok.at[owner, rows_of(p)],
            send_sem=help_send.at[0], recv_sem=tok_recv.at[1 + p],
            device_id={"blk": blk + aside}, device_id_type=MESH)

    sib_copy = pltpu.make_async_remote_copy(
        src_ref=tokens, dst_ref=tok.at[me], send_sem=tok_send.at[0], recv_sem=tok_recv.at[0],
        device_id={"shard": sib}, device_id_type=MESH)

    def send_direct(last):
        for p in range(last):
            for d in range(1, far + 1):
                direct(d, p).start()

    if helped:
        @pl.when(inner)
        def _():
            for p in range(PIECES - helped, PIECES):
                to_relay(p).start()
            send_direct(PIECES - helped)
    else:
        send_direct(PIECES)
    sib_copy.start()

    def w_copy(j):
        return pltpu.make_async_copy(
            w_hbm.at[:, pl.ds(pl.multiple_of(j * chunk, chunk), chunk)], w.at[j], load_sem.at[3 + j])

    tgt_copy = pltpu.make_async_copy(targets, tgt, load_sem.at[2])
    tgt_copy.start()
    for j in range(chunks):
        w_copy(j).start()

    def hidden_of(q, r0, n):
        def tile(t, c):
            cols = pl.ds(pl.multiple_of(t * UPTILE, UPTILE), UPTILE)
            v = silu(jnp.dot(tok[q, r0:r0 + n], up[:, cols], preferred_element_type=jnp.float32))
            hid[q, r0:r0 + n, cols] = v.astype(jnp.bfloat16)
            hidt[cols, pl.ds(pl.multiple_of(q * trows + r0, 128), n)] = v.T.astype(jnp.bfloat16)
            return c

        lax.fori_loop(0, ff // UPTILE, tile, 0, unroll=True)

    def rs_copy(j, i):
        return pltpu.make_async_remote_copy(
            src_ref=part.at[j, i - 1], dst_ref=rsl.at[j, i - 1],
            send_sem=rs_send.at[0], recv_sem=rs_recv.at[j],
            device_id={"shard": (me + i) % shards}, device_id_type=MESH)

    near = (sib - me + shards) % shards

    def out_of(q, j):
        return jnp.dot(hid[q], w[j], preferred_element_type=jnp.float32) * scale

    def give_out(j, i):
        part[j, i - 1] = out_of((me + i) % shards, j).astype(jnp.bfloat16)
        rs_copy(j, i).start()

    mid = trows // 2

    def give_half(i, r0):
        rows = slice(r0, r0 + mid)
        v = jnp.dot(hid[(me + i) % shards, rows], w[0], preferred_element_type=jnp.float32) * scale
        part[0, i - 1, rows] = v.astype(jnp.bfloat16)
        pltpu.make_async_remote_copy(
            src_ref=part.at[0, i - 1, pl.ds(r0, mid)], dst_ref=rsl.at[0, i - 1, pl.ds(r0, mid)],
            send_sem=rs_send.at[0], recv_sem=rs_recv.at[0],
            device_id={"shard": (me + i) % shards}, device_id_type=MESH).start()

    def far_half(base, d, r0):
        i = (base - 2 * d + 2 * shards) % shards
        hidden_of((me + i) % shards, r0, mid)
        give_half(i, r0)

    def out_away(j):
        def one(n, c):
            give_out(j, 1 + n + jnp.where(n + 1 >= near, 1, 0))
            return c

        lax.fori_loop(0, shards - 2, one, 0)

    def out_here(j):
        give_out(j, near)
        own[j % 4] = out_of(me, j)

    def relay_one(p):
        if helped:
            @pl.when(jnp.logical_not(inner))
            def _():
                to_relay(p).wait_recv()
                from_relay(p).start()

    def pass_on(pieces):
        for p in pieces:
            for d in range(1, far + 1):
                direct(d, p).wait_recv()
                forward(d, p).start()

    def passed_on(pieces):
        for p in pieces:
            for d in range(1, far + 1):
                forward(d, p).wait_recv()

    own_tok.wait()
    up_copy.wait()
    hidden_of(me, 0, trows)
    for p in range(PIECES - helped, PIECES - 1):
        relay_one(p)
    sib_copy.wait_recv()
    hidden_of(sib, 0, trows)
    if helped:
        relay_one(PIECES - 1)

        @pl.when(jnp.logical_not(inner))
        def _():
            send_direct(PIECES)

    h = PIECES // 2
    for j in range(EARLY):
        w_copy(j).wait()
        out_here(j)
        pass_on(range(h * j // EARLY, h * (j + 1) // EARLY))
    for d in range(1, far + 1):
        far_half(0, d, 0)
    passed_on(range(h))
    for d in range(1, far + 1):
        far_half(near, d, 0)
    pass_on(range(h, PIECES))
    for d in range(1, far + 1):
        far_half(0, d, mid)
    passed_on(range(h, PIECES))
    for d in range(1, far + 1):
        far_half(near, d, mid)

    tgt_copy.wait()

    def ag_copy(j, i):
        return pltpu.make_async_remote_copy(
            src_ref=res.at[j, me], dst_ref=res.at[j, me],
            send_sem=ag_send.at[0], recv_sem=ag_recv.at[j],
            device_id={"shard": (me + i) % shards}, device_id_type=MESH)

    def stage_resid(j):
        await_bytes(rsl.at[j], rs_recv.at[j])
        total = own[j % 4]
        for i in range(1, shards):
            total = total + rsl[j, i - 1].astype(jnp.float32)
        cols = pl.ds(pl.multiple_of(j * chunk, chunk), chunk)
        res[j, me] = (total - tgt[:, cols].astype(jnp.float32)).astype(jnp.bfloat16)
        for i in range(1, shards):
            ag_copy(j, i).start()

    def place(k):
        r = pl.ds(pl.multiple_of((k // cs) * pr, 16), pr)
        return r, (k % cs) * pc

    half = workers // 2
    mine = blk // half

    def peer(i):
        here = (i - 1) // half
        side = (mine + 1 + here) % 2
        return side * half + (blk + (i - 1) - here * (half - 1)) % half

    def a2a_copy(j, k, i):
        r, c0 = place(k)
        cols = pl.ds(0, pc) if cs == 1 else pl.ds(pl.multiple_of(c0, 128), pc)
        return pltpu.make_async_remote_copy(
            src_ref=w.at[j, r, cols], dst_ref=land.at[j, blk],
            send_sem=a2a_send.at[0], recv_sem=a2a_recv.at[j],
            device_id={"blk": k}, device_id_type=MESH)

    def stage_step(j):
        await_bytes(res.at[j, pl.ds(0, shards - 1)], ag_recv.at[j])

        def one(n, c):
            i = n + 1
            k = peer(i)
            r, c0 = place(k)
            cols = pl.ds(0, pc) if cs == 1 else pl.ds(pl.multiple_of(c0, 128), pc)
            rhs = res[j].reshape(shards * trows, chunk) if cs == 1 else (
                res[j, :, :, cols].reshape(shards * trows, pc))
            grad = jnp.dot(hidt[r, :], rhs, preferred_element_type=jnp.float32)
            new = (w[j, r, cols].astype(jnp.float32) - (learn_rate * scale) * grad).astype(jnp.bfloat16)

            @pl.when(i < workers)
            def _():
                w[j, r, cols] = new
                a2a_copy(j, k, i).start()

            @pl.when(i == workers)
            def _():
                land[j, blk] = new

            return c

        lax.fori_loop(0, workers, one, 0)

    def out_at(j, k):
        r, c0 = place(k)
        return out.at[r, pl.ds(pl.multiple_of(j * chunk + c0, 128), pc)]

    def ret_copy(j, i):
        k = peer(i)
        return pltpu.make_async_remote_copy(
            src_ref=land.at[j, k], dst_ref=out_at(j, blk),
            send_sem=ret_send.at[0], recv_sem=ret_recv.at[0],
            device_id={"blk": k}, device_id_type=MESH)

    def own_copy(j):
        return pltpu.make_async_copy(land.at[j, blk], out_at(j, blk), own_sem.at[0])

    rounds = numer.shape[1]

    def stage_mix(j):
        await_bytes(land.at[j, pl.ds(0, workers - 1)], a2a_recv.at[j])
        coef = [
            [[numer[e, r, k].astype(jnp.float32) * 0.25 for e in range(3)] for k in range(workers)]
            for r in range(rounds)
        ]

        def tile(t, c):
            rows = pl.ds(pl.multiple_of(t * ROWTILE, ROWTILE), ROWTILE)
            cur = [land[j, k, rows, :].astype(jnp.float32) for k in range(workers)]
            for r in range(rounds):
                cur = [
                    (
                        coef[r][k][0] * cur[k]
                        + coef[r][k][1] * cur[(k - 1) % workers]
                        + coef[r][k][2] * cur[(k + 1) % workers]
                    ).astype(jnp.bfloat16).astype(jnp.float32)
                    for k in range(workers)
                ]
            total = functools.reduce(lambda a, b: a + b, cur)
            average = total * jnp.float32(1.0 / workers)
            for k in range(workers):
                land[j, k, rows, :] = (cur[k] - average).astype(jnp.bfloat16)
            return c

        lax.fori_loop(0, pr // ROWTILE, tile, 0)

        def give(i, c):
            ret_copy(j, i).start()
            return c

        lax.fori_loop(1, workers, give, 0)
        own_copy(j).start()

    def step(t, c):
        @pl.when((t < chunks) & (t >= EARLY))
        def _():
            w_copy(t).wait()

        @pl.when((t >= 1) & (t < chunks))
        def _():
            out_away(t)

        @pl.when((t < chunks) & (t >= EARLY))
        def _():
            out_here(t)

        @pl.when((t >= 1) & (t - 1 < chunks))
        def _():
            stage_step(t - 1)

        @pl.when(t < chunks)
        def _():
            stage_resid(t)

        @pl.when(t >= LAG_MIX)
        def _():
            stage_mix(t - LAG_MIX)

        return c

    lax.fori_loop(0, chunks + LAG_MIX, step, 0)

    await_bytes(tok.at[pl.ds(0, 2 * far + 1)], tok_send.at[0])
    if helped:
        @pl.when(jnp.logical_not(inner))
        def _():
            await_bytes(relay, help_send.at[0])

    await_bytes(part, rs_send.at[0])
    await_bytes(res.at[:, pl.ds(0, shards - 1)], ag_send.at[0])
    away = land.at[:, pl.ds(0, workers - 1)]
    await_bytes(away, a2a_send.at[0])
    await_bytes(away, ret_send.at[0])
    await_bytes(away, ret_recv.at[0])
    await_bytes(land.at[:, 0], own_sem.at[0])


def solution(mesh):
    workers, shards = mesh.shape["blk"], mesh.shape["shard"]

    def body(tokens, targets, up_weight, down_weight, mix_numer):
        weight = down_weight[0]
        ff, d = weight.shape
        trows = tokens.shape[0]

        rs = math.gcd(workers, ff // 16)
        cs = workers // rs
        chunk = 128 * cs
        chunks = d // chunk
        pr, pc = ff // rs, chunk // cs
        far = shards // 2 - 1
        bf = jnp.bfloat16
        dma = pltpu.SemaphoreType.DMA
        any_ref = pl.BlockSpec(memory_space=pltpu.HBM)
        out = pl.pallas_call(
            functools.partial(kernel, workers, shards, rs, cs),
            out_shape=pltpu.VMEM((ff, d), bf),
            in_specs=[any_ref] * 4 + [pl.BlockSpec(memory_space=pltpu.SMEM)],
            out_specs=pl.BlockSpec(memory_space=pltpu.VMEM),
            scratch_shapes=[
                pltpu.VMEM((shards, trows, d), bf),
                pltpu.VMEM((d, ff), bf),
                pltpu.VMEM((chunks, ff, chunk), bf),
                pltpu.VMEM((trows, d), bf),
                pltpu.VMEM((shards, trows, ff), bf),
                pltpu.VMEM((ff, shards * trows), bf),
                pltpu.VMEM((4, trows, chunk), jnp.float32),
                pltpu.VMEM((chunks, shards - 1, trows, chunk), bf),
                pltpu.VMEM((chunks, shards - 1, trows, chunk), bf),
                pltpu.VMEM((chunks, shards, trows, chunk), bf),
                pltpu.VMEM((chunks, workers, pr, pc), bf),
                pltpu.VMEM((HELPED, trows // PIECES, d), bf),
                dma((3 + chunks,)),
                dma((1,)),
                dma((1 + 2 * far * PIECES,)),
                dma((1,)),
                dma((HELPED,)),
                dma((1,)),
                dma((chunks,)),
                dma((1,)),
                dma((chunks,)),
                dma((1,)),
                dma((chunks,)),
                dma((1,)),
                dma((1,)),
                dma((1,)),
            ],
            compiler_params=pltpu.CompilerParams(
                collective_id=0, has_side_effects=True, vmem_limit_bytes=54 * 1024 * 1000
            ),
        )(tokens, targets, up_weight, weight, jnp.transpose(mix_numer, (2, 0, 1)))
        return out[None]

    in_specs = (
        P(("blk", "shard"), None),
        P(("blk", "shard"), None),
        P(None, "shard"),
        P("blk", "shard", None),
        P(),
    )
    return jax.shard_map(
        body, mesh=mesh, in_specs=in_specs, out_specs=P("blk", "shard", None), check_vma=False
    )
```

```python
import functools
import math

import jax
import jax.numpy as jnp
from jax import lax
from jax.experimental import pallas as pl
from jax.experimental.pallas import tpu as pltpu
from jax.sharding import PartitionSpec as P

learn_rate = 2.0
MESH = pl.DeviceIdType.MESH
UPTILE = 256
LAG_MIX = 4
PIECES = 8
HELPED = 3
EARLY = 2
ROWTILE = 16


def silu(v):
    return v / (1.0 + jnp.exp(-v))


def kernel(
    workers, shards, rs, cs,
    tokens, targets, up_hbm, w_hbm, numer, out,
    tok, up, w, tgt, hid, hidt, own, part, rsl, res, land, relay,
    load_sem, tok_send, tok_recv, help_send, help_recv, rs_send, rs_recv, ag_send, ag_recv,
    a2a_send, a2a_recv, ret_send, ret_recv, own_sem,
):
    blk = lax.axis_index("blk")
    me = lax.axis_index("shard")
    sib = me + 1 - 2 * (me % 2)
    trows = tokens.shape[0]
    width = tokens.shape[1]
    ff = hidt.shape[0]
    chunks, chunk = w.shape[0], w.shape[2]
    pr, pc = ff // rs, chunk // cs
    far = shards // 2 - 1
    scale = jnp.float32(1.0 / math.sqrt(ff * shards))

    own_tok = pltpu.make_async_copy(tokens, tok.at[me], load_sem.at[0])
    own_tok.start()
    up_copy = pltpu.make_async_copy(up_hbm, up, load_sem.at[1])
    up_copy.start()

    barrier = pltpu.get_barrier_semaphore()

    def await_bytes(ref, sem):
        pltpu.make_async_copy(ref, ref, sem).wait()

    def greet_blk(i, c):
        pl.semaphore_signal(
            barrier, inc=1, device_id={"blk": (blk + i) % workers}, device_id_type=MESH)
        return c

    lax.fori_loop(1, workers, greet_blk, 0)
    for i in range(1, shards):
        pl.semaphore_signal(
            barrier, inc=1, device_id={"shard": (me + i) % shards}, device_id_type=MESH)
    quarter = workers // 4
    helped = HELPED if workers % 4 == 0 and far == 1 else 0
    inner = (blk >= quarter) & (blk < workers - quarter)
    aside = jnp.where(blk < workers // 2, quarter, -quarter)
    helper = {"blk": blk + jnp.where(inner, -aside, aside), "shard": (me + 2) % shards}
    if helped:
        pl.semaphore_signal(barrier, inc=1, device_id=helper, device_id_type=MESH)
    pl.semaphore_wait(barrier, workers - 1 + shards - 1 + (1 if helped else 0))

    prow = trows // PIECES

    def rows_of(p):
        return pl.ds(p * prow, prow)

    def tok_copy(src, sem, owner, p, to):
        return pltpu.make_async_remote_copy(
            src_ref=src.at[rows_of(p)], dst_ref=tok.at[owner, rows_of(p)],
            send_sem=tok_send.at[0], recv_sem=tok_recv.at[sem],
            device_id={"shard": to}, device_id_type=MESH)

    def direct(d, p):
        return tok_copy(tokens, 1 + (2 * d - 2) * PIECES + p, me, p, (me + 2 * d) % shards)

    def forward(d, p):
        src = (me - 2 * d + 2 * shards) % shards
        return tok_copy(tok.at[src], 1 + (2 * d - 1) * PIECES + p, src, p, sib)

    def to_relay(p):
        return pltpu.make_async_remote_copy(
            src_ref=tokens.at[rows_of(p)], dst_ref=relay.at[p - PIECES + helped],
            send_sem=tok_send.at[0], recv_sem=help_recv.at[p - PIECES + helped],
            device_id=helper, device_id_type=MESH)

    def from_relay(p):
        owner = (me + 2) % shards
        return pltpu.make_async_remote_copy(
            src_ref=relay.at[p - PIECES + helped], dst_ref=tok.at[owner, rows_of(p)],
            send_sem=help_send.at[0], recv_sem=tok_recv.at[1 + p],
            device_id={"blk": blk + aside}, device_id_type=MESH)

    sib_copy = pltpu.make_async_remote_copy(
        src_ref=tokens, dst_ref=tok.at[me], send_sem=tok_send.at[0], recv_sem=tok_recv.at[0],
        device_id={"shard": sib}, device_id_type=MESH)

    def send_direct(last):
        for p in range(last):
            for d in range(1, far + 1):
                direct(d, p).start()

    if helped:
        @pl.when(inner)
        def _():
            for p in range(PIECES - helped, PIECES):
                to_relay(p).start()
            send_direct(PIECES - helped)
    else:
        send_direct(PIECES)
    sib_copy.start()

    def w_copy(j):
        return pltpu.make_async_copy(
            w_hbm.at[:, pl.ds(pl.multiple_of(j * chunk, chunk), chunk)], w.at[j], load_sem.at[3 + j])

    tgt_copy = pltpu.make_async_copy(targets, tgt, load_sem.at[2])
    tgt_copy.start()
    for j in range(chunks):
        w_copy(j).start()

    def hidden_of(q, r0, n):
        def tile(t, c):
            cols = pl.ds(pl.multiple_of(t * UPTILE, UPTILE), UPTILE)
            v = silu(jnp.dot(tok[q, r0:r0 + n], up[:, cols], preferred_element_type=jnp.float32))
            hid[q, r0:r0 + n, cols] = v.astype(jnp.bfloat16)
            hidt[cols, pl.ds(pl.multiple_of(q * trows + r0, 128), n)] = v.T.astype(jnp.bfloat16)
            return c

        lax.fori_loop(0, ff // UPTILE, tile, 0, unroll=True)

    def rs_copy(j, i):
        return pltpu.make_async_remote_copy(
            src_ref=part.at[j, i - 1], dst_ref=rsl.at[j, i - 1],
            send_sem=rs_send.at[0], recv_sem=rs_recv.at[jnp.where(j == 0, chunks, j)],
            device_id={"shard": (me + i) % shards}, device_id_type=MESH)

    near = (sib - me + shards) % shards

    def out_of(q, j):
        return jnp.dot(hid[q], w[j], preferred_element_type=jnp.float32) * scale

    def give_out(j, i):
        part[j, i - 1] = out_of((me + i) % shards, j).astype(jnp.bfloat16)
        rs_copy(j, i).start()

    mid = trows // 2

    def give_half(i, r0):
        rows = slice(r0, r0 + mid)
        v = jnp.dot(hid[(me + i) % shards, rows], w[0], preferred_element_type=jnp.float32) * scale
        part[0, i - 1, rows] = v.astype(jnp.bfloat16)
        pltpu.make_async_remote_copy(
            src_ref=part.at[0, i - 1, pl.ds(r0, mid)], dst_ref=rsl.at[0, i - 1, pl.ds(r0, mid)],
            send_sem=rs_send.at[0], recv_sem=rs_recv.at[chunks if r0 == 0 else 0],
            device_id={"shard": (me + i) % shards}, device_id_type=MESH).start()

    def far_half(base, d, r0):
        i = (base - 2 * d + 2 * shards) % shards
        hidden_of((me + i) % shards, r0, mid)
        give_half(i, r0)

    def out_away(j):
        def one(n, c):
            give_out(j, 1 + n + jnp.where(n + 1 >= near, 1, 0))
            return c

        lax.fori_loop(0, shards - 2, one, 0)

    def out_here(j):
        give_out(j, near)
        own[j % 4] = out_of(me, j)

    def relay_one(p):
        if helped:
            @pl.when(jnp.logical_not(inner))
            def _():
                to_relay(p).wait_recv()
                from_relay(p).start()

    def pass_on(pieces):
        for p in pieces:
            for d in range(1, far + 1):
                direct(d, p).wait_recv()
                forward(d, p).start()

    def passed_on(pieces):
        for p in pieces:
            for d in range(1, far + 1):
                forward(d, p).wait_recv()

    own_tok.wait()
    up_copy.wait()
    hidden_of(me, 0, trows)
    for p in range(PIECES - helped, PIECES - 1):
        relay_one(p)
    sib_copy.wait_recv()
    hidden_of(sib, 0, trows)
    if helped:
        relay_one(PIECES - 1)

        @pl.when(jnp.logical_not(inner))
        def _():
            send_direct(PIECES)

    h = PIECES // 2
    for j in range(EARLY):
        w_copy(j).wait()
        out_here(j)
        pass_on(range(h * j // EARLY, h * (j + 1) // EARLY))
    for d in range(1, far + 1):
        far_half(0, d, 0)
    passed_on(range(h))
    for d in range(1, far + 1):
        far_half(near, d, 0)
    pass_on(range(h, PIECES))
    for d in range(1, far + 1):
        far_half(0, d, mid)
    passed_on(range(h, PIECES))
    for d in range(1, far + 1):
        far_half(near, d, mid)

    tgt_copy.wait()

    def ag_copy(j, i):
        return pltpu.make_async_remote_copy(
            src_ref=res.at[j, me], dst_ref=res.at[j, me],
            send_sem=ag_send.at[0], recv_sem=ag_recv.at[j],
            device_id={"shard": (me + i) % shards}, device_id_type=MESH)

    def stage_resid(j):
        await_bytes(rsl.at[j], rs_recv.at[j])
        total = own[j % 4]
        for i in range(1, shards):
            total = total + rsl[j, i - 1].astype(jnp.float32)
        cols = pl.ds(pl.multiple_of(j * chunk, chunk), chunk)
        res[j, me] = (total - tgt[:, cols].astype(jnp.float32)).astype(jnp.bfloat16)
        for i in range(1, shards):
            ag_copy(j, i).start()

    def resid_half(r0):
        if r0 == 0:
            await_bytes(rsl.at[0, pl.ds(0, shards // 2)], rs_recv.at[chunks])
        else:
            await_bytes(rsl.at[0, pl.ds(0, far)], rs_recv.at[0])
        rows = slice(r0, r0 + mid)
        total = own[0, rows]
        for i in range(1, shards):
            total = total + rsl[0, i - 1, rows].astype(jnp.float32)
        res[0, me, rows] = (total - tgt[rows, 0:chunk].astype(jnp.float32)).astype(jnp.bfloat16)
        for i in range(1, shards):
            pltpu.make_async_remote_copy(
                src_ref=res.at[0, me, pl.ds(r0, mid)], dst_ref=res.at[0, me, pl.ds(r0, mid)],
                send_sem=ag_send.at[0], recv_sem=ag_recv.at[0],
                device_id={"shard": (me + i) % shards}, device_id_type=MESH).start()

    def place(k):
        r = pl.ds(pl.multiple_of((k // cs) * pr, 16), pr)
        return r, (k % cs) * pc

    half = workers // 2
    mine = blk // half

    def peer(i):
        here = (i - 1) // half
        side = (mine + 1 + here) % 2
        return side * half + (blk + (i - 1) - here * (half - 1)) % half

    def a2a_copy(j, k, i):
        r, c0 = place(k)
        cols = pl.ds(0, pc) if cs == 1 else pl.ds(pl.multiple_of(c0, 128), pc)
        return pltpu.make_async_remote_copy(
            src_ref=w.at[j, r, cols], dst_ref=land.at[j, blk],
            send_sem=a2a_send.at[0], recv_sem=a2a_recv.at[j],
            device_id={"blk": k}, device_id_type=MESH)

    def stage_step(j):
        await_bytes(res.at[j, pl.ds(0, shards - 1)], ag_recv.at[j])

        def one(n, c):
            i = n + 1
            k = peer(i)
            r, c0 = place(k)
            cols = pl.ds(0, pc) if cs == 1 else pl.ds(pl.multiple_of(c0, 128), pc)
            rhs = res[j].reshape(shards * trows, chunk) if cs == 1 else (
                res[j, :, :, cols].reshape(shards * trows, pc))
            grad = jnp.dot(hidt[r, :], rhs, preferred_element_type=jnp.float32)
            new = (w[j, r, cols].astype(jnp.float32) - (learn_rate * scale) * grad).astype(jnp.bfloat16)

            @pl.when(i < workers)
            def _():
                w[j, r, cols] = new
                a2a_copy(j, k, i).start()

            @pl.when(i == workers)
            def _():
                land[j, blk] = new

            return c

        lax.fori_loop(0, workers, one, 0)

    def out_at(j, k):
        r, c0 = place(k)
        return out.at[r, pl.ds(pl.multiple_of(j * chunk + c0, 128), pc)]

    def ret_copy(j, i):
        k = peer(i)
        return pltpu.make_async_remote_copy(
            src_ref=land.at[j, k], dst_ref=out_at(j, blk),
            send_sem=ret_send.at[0], recv_sem=ret_recv.at[0],
            device_id={"blk": k}, device_id_type=MESH)

    def own_copy(j):
        return pltpu.make_async_copy(land.at[j, blk], out_at(j, blk), own_sem.at[0])

    rounds = numer.shape[1]

    def stage_mix(j):
        await_bytes(land.at[j, pl.ds(0, workers - 1)], a2a_recv.at[j])
        coef = [
            [[numer[e, r, k].astype(jnp.float32) * 0.25 for e in range(3)] for k in range(workers)]
            for r in range(rounds)
        ]

        def tile(t, c):
            rows = pl.ds(pl.multiple_of(t * ROWTILE, ROWTILE), ROWTILE)
            cur = [land[j, k, rows, :].astype(jnp.float32) for k in range(workers)]
            for r in range(rounds):
                cur = [
                    (
                        coef[r][k][0] * cur[k]
                        + coef[r][k][1] * cur[(k - 1) % workers]
                        + coef[r][k][2] * cur[(k + 1) % workers]
                    ).astype(jnp.bfloat16).astype(jnp.float32)
                    for k in range(workers)
                ]
            total = functools.reduce(lambda a, b: a + b, cur)
            average = total * jnp.float32(1.0 / workers)
            for k in range(workers):
                land[j, k, rows, :] = (cur[k] - average).astype(jnp.bfloat16)
            return c

        lax.fori_loop(0, pr // ROWTILE, tile, 0)

        def give(i, c):
            ret_copy(j, i).start()
            return c

        lax.fori_loop(1, workers, give, 0)
        own_copy(j).start()

    def step(t, c):
        @pl.when((t < chunks) & (t >= EARLY))
        def _():
            w_copy(t).wait()

        @pl.when((t >= 1) & (t < chunks))
        def _():
            out_away(t)

        @pl.when((t < chunks) & (t >= EARLY))
        def _():
            out_here(t)

        @pl.when((t >= 1) & (t - 1 < chunks))
        def _():
            stage_step(t - 1)

        @pl.when((t >= 1) & (t < chunks))
        def _():
            stage_resid(t)

        @pl.when(t >= LAG_MIX)
        def _():
            stage_mix(t - LAG_MIX)

        return c

    resid_half(0)
    resid_half(mid)
    lax.fori_loop(0, chunks + LAG_MIX, step, 0)

    await_bytes(tok.at[pl.ds(0, 2 * far + 1)], tok_send.at[0])
    if helped:
        @pl.when(jnp.logical_not(inner))
        def _():
            await_bytes(relay, help_send.at[0])

    await_bytes(part, rs_send.at[0])
    await_bytes(res.at[:, pl.ds(0, shards - 1)], ag_send.at[0])
    away = land.at[:, pl.ds(0, workers - 1)]
    await_bytes(away, a2a_send.at[0])
    await_bytes(away, ret_send.at[0])
    await_bytes(away, ret_recv.at[0])
    await_bytes(land.at[:, 0], own_sem.at[0])


def solution(mesh):
    workers, shards = mesh.shape["blk"], mesh.shape["shard"]

    def body(tokens, targets, up_weight, down_weight, mix_numer):
        weight = down_weight[0]
        ff, d = weight.shape
        trows = tokens.shape[0]

        rs = math.gcd(workers, ff // 16)
        cs = workers // rs
        chunk = 128 * cs
        chunks = d // chunk
        pr, pc = ff // rs, chunk // cs
        far = shards // 2 - 1
        bf = jnp.bfloat16
        dma = pltpu.SemaphoreType.DMA
        any_ref = pl.BlockSpec(memory_space=pltpu.HBM)
        out = pl.pallas_call(
            functools.partial(kernel, workers, shards, rs, cs),
            out_shape=pltpu.VMEM((ff, d), bf),
            in_specs=[any_ref] * 4 + [pl.BlockSpec(memory_space=pltpu.SMEM)],
            out_specs=pl.BlockSpec(memory_space=pltpu.VMEM),
            scratch_shapes=[
                pltpu.VMEM((shards, trows, d), bf),
                pltpu.VMEM((d, ff), bf),
                pltpu.VMEM((chunks, ff, chunk), bf),
                pltpu.VMEM((trows, d), bf),
                pltpu.VMEM((shards, trows, ff), bf),
                pltpu.VMEM((ff, shards * trows), bf),
                pltpu.VMEM((4, trows, chunk), jnp.float32),
                pltpu.VMEM((chunks, shards - 1, trows, chunk), bf),
                pltpu.VMEM((chunks, shards - 1, trows, chunk), bf),
                pltpu.VMEM((chunks, shards, trows, chunk), bf),
                pltpu.VMEM((chunks, workers, pr, pc), bf),
                pltpu.VMEM((HELPED, trows // PIECES, d), bf),
                dma((3 + chunks,)),
                dma((1,)),
                dma((1 + 2 * far * PIECES,)),
                dma((1,)),
                dma((HELPED,)),
                dma((1,)),
                dma((chunks + 1,)),
                dma((1,)),
                dma((chunks,)),
                dma((1,)),
                dma((chunks,)),
                dma((1,)),
                dma((1,)),
                dma((1,)),
            ],
            compiler_params=pltpu.CompilerParams(
                collective_id=0, has_side_effects=True, vmem_limit_bytes=54 * 1024 * 1000
            ),
        )(tokens, targets, up_weight, weight, jnp.transpose(mix_numer, (2, 0, 1)))
        return out[None]

    in_specs = (
        P(("blk", "shard"), None),
        P(("blk", "shard"), None),
        P(None, "shard"),
        P("blk", "shard", None),
        P(),
    )
    return jax.shard_map(
        body, mesh=mesh, in_specs=in_specs, out_specs=P("blk", "shard", None), check_vma=False
    )
```
